32 devices in a mesh: px: 2 (over core), pz: 16 (over z, y, x).
Axes of the slice: x: 2, y: 2, z: 4, core: 2. Of those that a mesh axis runs over, the one named last changes fastest.
Arguments:
- velocity: float32 [3, 256, 32, 256], P(None, 'pz', None, 'px'), may hold values from -8 to 8, as said below
- filter_inverse: float32 [256, 256], replicated, may hold values from 0 to 2, as said below
- filter_block: int32 [256], replicated, may hold values from 0 to 7, never falling along the last dimension, each value on 1 to 128 neighbouring positions
- plane_bin: int32 [256], replicated, may hold values from 0 to 63, never falling along the last dimension, each value on 1 to 16 neighbouring positions
Outputs:
- leonard: float32 [6, 256, 32, 256], P(None, 'pz', None, 'px')
- viscosity: float32 [256, 32, 256], P('pz', None, 'px')
- coefficient: float32 [256], replicated
The draws below stay inside these ranges and needn't reach their ends.
Inputs may be any that keep to these rules, and one draw needn't show every extreme that they name: `velocity`: each component is a rough random field. `filter_inverse`: entries are positive. `filter_block`: never falls along the planes; each of the 8 blocks holds 1 to 128 consecutive planes, one exactly 128. `plane_bin`: never falls along the planes; each of the 64 bins holds 1 to 16 consecutive planes, one exactly 16.
All inputs are finite; a program needn't handle non-finite values.
Results may differ from the reference program's by a relative error of at most 0.0003.
Values sent between devices are 32-bit elements; how exact they have to be, the bound alone decides.
A program may use at most 128 MiB of HBM per device.

```python
import math
import jax
import jax.numpy as jnp
import numpy as np
from jax import lax

NY = 256
NFB = 8
FBMOST = 128
NBIN = 64
BINMOST = 16
NX = 256
NZ = 32


def draw_velocity(key, part):
    noise_key, scale_key = jax.random.split(jax.random.fold_in(key, 11))
    base = jax.random.normal(noise_key, (3, NY, NZ, NX), jnp.float32)
    amplitude = jnp.exp(jax.random.uniform(scale_key, (1, 1, NZ, NX // 8), jnp.float32, -0.7, 0.7))
    amplitude = jnp.repeat(amplitude, 8, axis=3)
    return jnp.clip(base * amplitude, -8.0, 8.0)


def draw_filter_inverse(key, part):
    entry_key = jax.random.fold_in(key, 23)
    rows = jnp.arange(NY, dtype=jnp.float32)
    distance = jnp.abs(rows[:, None] - rows[None, :])
    factors = jax.random.uniform(entry_key, (NY, NY), jnp.float32, 0.5, 1.5)
    return jnp.exp(-distance / 256.0) * factors


def split_up(number_of, total, bound, slope):
    loads = [(1 << 20) // math.isqrt(grade ** slope) + 1 for grade in range(2, number_of + 1)]
    spare, holding = total - bound - (number_of - 1), [1] * (number_of - 1)
    while spare > 0:
        free = [i for i in range(number_of - 1) if holding[i] < bound]
        whole, budget = sum([loads[i] for i in free]), spare
        for i in free:
            extra = min(bound - holding[i], max(1, budget * loads[i] // whole), spare)
            holding[i] = holding[i] + extra
            spare = spare - extra
    return np.array([bound] + holding)


def ragged_sizes(rng, count, total, reach, lean):
    if count == 2:
        one = jax.random.randint(rng, (), max(1, total - reach), min(reach, total - 1) + 1)
        return jnp.stack([one, total - one])
    sizes = jnp.asarray(split_up(count, total, reach, lean), jnp.int32)
    couples = (count - 1) // 2
    donor, sink = sizes[1:1 + 2 * couples:2], sizes[2:2 + 2 * couples:2]
    room = jnp.minimum(donor - 1, reach - sink)
    shifted = jax.random.randint(jax.random.fold_in(rng, 1), (couples,), 0, 1 << 20) % (room + 1)
    sizes = sizes.at[1:1 + 2 * couples:2].set(donor - shifted).at[2:2 + 2 * couples:2].set(sink + shifted)
    return sizes[jax.random.permutation(jax.random.fold_in(rng, 2), count)]


def setup_inputs(seed: int = 0) -> dict:
    keys = jax.random.split(jax.random.key(seed), 5)
    velocity = draw_velocity(jax.random.fold_in(keys[4], 71), 0)
    filter_inverse = draw_filter_inverse(jax.random.fold_in(keys[4], 71), 0)
    filter_block = jnp.searchsorted(jnp.cumsum(ragged_sizes(keys[2], NFB, NY, FBMOST, 1)), jnp.arange(NY), side="right").astype(jnp.int32)
    plane_bin = jnp.searchsorted(jnp.cumsum(ragged_sizes(keys[3], NBIN, NY, BINMOST, 1)), jnp.arange(NY), side="right").astype(jnp.int32)
    return dict(velocity=velocity, filter_inverse=filter_inverse, filter_block=filter_block, plane_bin=plane_bin)


def block_weights(filter_inverse, filter_block):
    same = (filter_block[:, None] == filter_block[None, :]).astype(jnp.float32)
    masked = filter_inverse * same
    return masked / lax.optimization_barrier(jnp.sum(masked, axis=1, keepdims=True))

def quantities(padded):
    centre = padded[:, 1:-1, 1:-1, 1:-1]
    along_y = (padded[:, 2:, 1:-1, 1:-1] - padded[:, :-2, 1:-1, 1:-1]) * 0.5
    along_z = (padded[:, 1:-1, 2:, 1:-1] - padded[:, 1:-1, :-2, 1:-1]) * 0.5
    along_x = (padded[:, 1:-1, 1:-1, 2:] - padded[:, 1:-1, 1:-1, :-2]) * 0.5
    strain = jnp.stack([along_x[0], along_y[1], along_z[2], 0.5 * (along_y[0] + along_x[1]), 0.5 * (along_z[0] + along_x[2]), 0.5 * (along_z[1] + along_y[2])])
    magnitude = jnp.sqrt(2.0 * lax.optimization_barrier(jnp.sum(strain[:3] * strain[:3], axis=0)) + 4.0 * lax.optimization_barrier(jnp.sum(strain[3:] * strain[3:], axis=0)))
    products = jnp.stack([centre[0] * centre[0], centre[1] * centre[1], centre[2] * centre[2], centre[0] * centre[1], centre[0] * centre[2], centre[1] * centre[2]])
    fields = jnp.concatenate([centre, strain, products, magnitude[None] * strain], axis=0)
    along = (fields[..., :-2] + 2.0 * fields[..., 1:-1] + fields[..., 2:]) * 0.25
    boxed = (along[:, :, :-2] + 2.0 * along[:, :, 1:-1] + along[:, :, 2:]) * 0.25
    return (boxed, magnitude[:, 1:-1, 1:-1])

def contract(filtered):
    speed = filtered[0:3]
    strain = filtered[3:9]
    products = filtered[9:15]
    scaled = filtered[15:21]
    leonard = products - jnp.stack([speed[0] * speed[0], speed[1] * speed[1], speed[2] * speed[2], speed[0] * speed[1], speed[0] * speed[2], speed[1] * speed[2]])
    fmag = jnp.sqrt(2.0 * lax.optimization_barrier(jnp.sum(strain[:3] * strain[:3], axis=0)) + 4.0 * lax.optimization_barrier(jnp.sum(strain[3:] * strain[3:], axis=0)))
    model = scaled - 4.0 * fmag[None] * strain
    weights = jnp.array([1.0, 1.0, 1.0, 2.0, 2.0, 2.0], jnp.float32).reshape(6, 1, 1, 1)
    product_lm = lax.optimization_barrier(jnp.sum(weights * leonard * model, axis=0))
    product_mm = lax.optimization_barrier(jnp.sum(weights * model * model, axis=0))
    return (leonard, product_lm, product_mm)

def reference(velocity, filter_inverse, filter_block, plane_bin):
    weights = block_weights(filter_inverse, filter_block)

    def one_plane(plane):
        indices = ((plane + jnp.arange(-2, 3, dtype=jnp.int32)) % NZ).astype(jnp.int32)
        window = jnp.take(velocity, indices, axis=2)
        window = jnp.pad(window, ((0, 0), (1, 1), (0, 0), (0, 0)))
        window = jnp.concatenate([window[..., -2:], window, window[..., :2]], axis=3)
        boxed, magnitude = quantities(window)
        filtered = jnp.einsum('ab,kbzx->kazx', weights, boxed, precision=lax.Precision.HIGHEST)
        leonard, product_lm, product_mm = contract(filtered)
        return (leonard[:, :, 0, :], lax.optimization_barrier(jnp.sum(product_lm, axis=(1, 2))), lax.optimization_barrier(jnp.sum(product_mm, axis=(1, 2))), magnitude[:, 0, :])
    leonard, plane_lm, plane_mm, magnitude = lax.map(one_plane, jnp.arange(NZ, dtype=jnp.int32))
    plane_lm = lax.optimization_barrier(jnp.sum(plane_lm, axis=0))
    plane_mm = lax.optimization_barrier(jnp.sum(plane_mm, axis=0))
    onehot = (plane_bin[:, None] == jnp.arange(NBIN, dtype=jnp.int32)[None, :]).astype(jnp.float32)
    numer = jnp.dot(plane_lm, onehot, precision=lax.Precision.HIGHEST)
    denom = jnp.dot(plane_mm, onehot, precision=lax.Precision.HIGHEST)
    per_bin = numer / jnp.maximum(denom, jnp.float32(NX * NZ))
    coefficient = jnp.dot(onehot, per_bin, precision=lax.Precision.HIGHEST)
    leonard = jnp.transpose(leonard, (1, 2, 0, 3))
    viscosity = coefficient[:, None, None] * jnp.transpose(magnitude, (1, 0, 2))
    return (leonard, viscosity, coefficient)
```

```python
import functools

import jax
import jax.numpy as jnp
from jax import lax
from jax.experimental import pallas as pl
from jax.experimental.pallas import tpu as pltpu
from jax.sharding import PartitionSpec as P

NBIN = 64
PAIRS = ((0, 0), (1, 1), (2, 2), (0, 1), (0, 2), (1, 2))


def tensor_norm(s):
    diag = s[0] * s[0] + s[1] * s[1] + s[2] * s[2]
    off = s[3] * s[3] + s[4] * s[4] + s[5] * s[5]
    return jnp.sqrt(2.0 * diag + 4.0 * off)


def column_kernel(dims, own, right, left, weights, onehot_t, back, sums, ext, bhi, blo, filt, lms, mms, whi, wlo):
    n, win, lp, nx = dims
    zs = win - 4
    ny = n * lp
    lanes = 2 * nx
    lane = lax.broadcasted_iota(jnp.int32, (lp, nx), 1)
    from_right = lane < nx // 2

    heavy = weights[...].astype(jnp.bfloat16)
    whi[...] = heavy
    wlo[...] = (weights[...] - heavy.astype(jnp.float32)).astype(jnp.bfloat16)

    zero = jnp.zeros((8, lanes), jnp.float32)
    for c in range(3):
        for z in range(win):
            ext[c, z, 0:8, :] = zero
            ext[c, z, ny + 8 : ny + 16, :] = zero

    @pl.loop(0, n)
    def _(p):
        rows = pl.ds(pl.multiple_of(8 + p * lp, 8), lp)
        for c in range(3):
            for z in range(win):
                ext[c, z, rows, 0:nx] = own[p, c, z]
                ext[c, z, rows, nx:lanes] = jnp.where(from_right, right[p, c, z], left[p, c, z])

    @pl.loop(0, n)
    def _(p):
        base = pl.multiple_of(p * lp, 8)
        u = [[ext[c, z, pl.ds(base + 8, lp), :] for z in range(win)] for c in range(3)]
        boxes = [[None] * 21 for _ in range(zs)]
        for z in range(1, win - 1):
            v = [u[c][z] for c in range(3)]
            dx, dy, dz = [], [], []
            for c in range(3):
                dx.append(pltpu.roll(v[c], lanes - 1, 1) - pltpu.roll(v[c], 1, 1))
                tall = ext[c, z, pl.ds(base, lp + 16), :]
                dy.append(tall[9 : 9 + lp] - tall[7 : 7 + lp])
                dz.append(u[c][z + 1] - u[c][z - 1])
            s = [
                dx[0] * 0.5,
                dy[1] * 0.5,
                dz[2] * 0.5,
                0.25 * (dy[0] + dx[1]),
                0.25 * (dz[0] + dx[2]),
                0.25 * (dz[1] + dy[2]),
            ]
            mag = tensor_norm(s)
            fields = v + s + [v[i] * v[j] for i, j in PAIRS] + [mag * t for t in s]
            if 2 <= z < win - 2:
                back[p, 6, z - 2] = mag[:, :nx]
            for o in range(zs):
                step = z - (o + 2)
                if -1 <= step <= 1:
                    for k in range(21):
                        term = fields[k] if step else 2.0 * fields[k]
                        boxes[o][k] = term if boxes[o][k] is None else boxes[o][k] + term
        for o in range(zs):
            for k in range(21):
                f = boxes[o][k]
                box = (pltpu.roll(f, 1, 1) + pltpu.roll(f, lanes - 1, 1) + 2.0 * f)[:, :nx] * 0.0625
                high = box.astype(jnp.bfloat16)
                cols = slice(o * nx, (o + 1) * nx)
                bhi[k, pl.ds(base, lp), cols] = high
                blo[k, pl.ds(base, lp), cols] = (box - high.astype(jnp.float32)).astype(jnp.bfloat16)

    @pl.loop(0, 21)
    def _(k):
        dot = functools.partial(jnp.dot, preferred_element_type=jnp.float32)
        filt[k] = dot(whi[...], bhi[k]) + (dot(whi[...], blo[k]) + dot(wlo[...], bhi[k]))

    @pl.loop(0, n)
    def _(p):
        base = pl.multiple_of(p * lp, 8)
        lm_total = jnp.zeros((lp, nx), jnp.float32)
        mm_total = jnp.zeros((lp, nx), jnp.float32)
        for o in range(zs):
            g = [filt[k, pl.ds(base, lp), o * nx : (o + 1) * nx] for k in range(21)]
            fmag = 4.0 * tensor_norm(g[3:9])
            for q, (i, j) in enumerate(PAIRS):
                leonard = g[9 + q] - g[i] * g[j]
                model = g[15 + q] - fmag * g[3 + q]
                weighted = model if q < 3 else 2.0 * model
                lm_total += leonard * weighted
                mm_total += model * weighted
                back[p, q, o] = leonard
        lms[pl.ds(base, lp), :] = lm_total
        mms[pl.ds(base, lp), :] = mm_total

    dot = functools.partial(jnp.dot, preferred_element_type=jnp.float32, precision=lax.Precision.HIGHEST)
    sums[0] = dot(onehot_t[...], lms[...])
    sums[1] = dot(onehot_t[...], mms[...])


def local(velocity, filter_inverse, filter_block, plane_bin):
    _, lp, nz, nx = velocity.shape
    n = lax.axis_size("pz")
    m = lax.axis_size("px")
    ny, zs = n * lp, nz // n
    win = zs + 4

    same = (filter_block[:, None] == filter_block[None, :]).astype(jnp.float32)
    masked = filter_inverse * same
    weights = masked / jnp.sum(masked, axis=1, keepdims=True)
    onehot = (plane_bin[:, None] == jnp.arange(NBIN, dtype=jnp.int32)[None, :]).astype(jnp.float32)

    turned = jnp.transpose(velocity, (0, 2, 1, 3))
    turned = jnp.concatenate([turned[:, -2:], turned, turned[:, :2]], axis=1)
    sent = jnp.stack([turned[:, t * zs : t * zs + win] for t in range(n)])
    own = lax.all_to_all(sent, "pz", split_axis=0, concat_axis=0, tiled=True)
    right = lax.ppermute(own, "px", [((i + 1) % m, i) for i in range(m)])
    left = right if m == 2 else lax.ppermute(own, "px", [(i, (i + 1) % m) for i in range(m)])

    back, sums = pl.pallas_call(
        functools.partial(column_kernel, (n, win, lp, nx)),
        out_shape=(
            jax.ShapeDtypeStruct((n, 7, zs, lp, nx), jnp.float32),
            jax.ShapeDtypeStruct((2, NBIN, nx), jnp.float32),
        ),
        in_specs=[pl.BlockSpec(memory_space=pltpu.VMEM)] * 5,
        out_specs=(pl.BlockSpec(memory_space=pltpu.VMEM),) * 2,
        scratch_shapes=[
            pltpu.VMEM((3, win, ny + 16, 2 * nx), jnp.float32),
            pltpu.VMEM((21, ny, zs * nx), jnp.bfloat16),
            pltpu.VMEM((21, ny, zs * nx), jnp.bfloat16),
            pltpu.VMEM((21, ny, zs * nx), jnp.float32),
            pltpu.VMEM((ny, nx), jnp.float32),
            pltpu.VMEM((ny, nx), jnp.float32),
            pltpu.VMEM((ny, ny), jnp.bfloat16),
            pltpu.VMEM((ny, ny), jnp.bfloat16),
        ],
        compiler_params=pltpu.CompilerParams(vmem_limit_bytes=60 * 1024 * 1024),
    )(own, right, left, weights, onehot.T)

    numer, denom = lax.psum(jnp.sum(sums, axis=2), ("px", "pz"))
    cells = nx * m * nz
    per_bin = numer / jnp.maximum(denom, jnp.float32(cells))
    coefficient = jnp.dot(onehot, per_bin, precision=lax.Precision.HIGHEST)

    home = lax.all_to_all(back, "pz", split_axis=0, concat_axis=0, tiled=True)
    home = jnp.transpose(home, (1, 3, 0, 2, 4)).reshape(7, lp, nz, nx)
    local_coef = lax.dynamic_slice_in_dim(coefficient, lax.axis_index("pz") * lp, lp, 0)
    viscosity = local_coef[:, None, None] * home[6]
    return (home[:6], viscosity, coefficient)


def solution(mesh):
    return jax.shard_map(
        local,
        mesh=mesh,
        in_specs=(P(None, "pz", None, "px"), P(), P(), P()),
        out_specs=(P(None, "pz", None, "px"), P("pz", None, "px"), P()),
        check_vma=False,
    )
```

```python
import functools

import jax
import jax.numpy as jnp
from jax import lax
from jax.experimental import pallas as pl
from jax.experimental.pallas import tpu as pltpu
from jax.sharding import PartitionSpec as P

NBIN = 64
PAIRS = ((0, 0), (1, 1), (2, 2), (0, 1), (0, 2), (1, 2))


def tensor_norm(s):
    diag = s[0] * s[0] + s[1] * s[1] + s[2] * s[2]
    off = s[3] * s[3] + s[4] * s[4] + s[5] * s[5]
    return jnp.sqrt(2.0 * diag + 4.0 * off)


def strain_of(dx, dy, dz):
    return [
        dx[0] * 0.5,
        dy[1] * 0.5,
        dz[2] * 0.5,
        0.25 * (dy[0] + dx[1]),
        0.25 * (dz[0] + dx[2]),
        0.25 * (dz[1] + dy[2]),
    ]


def fill_from_blocks(dims, ext, own, right, left):
    n, win, lp, nx = dims
    lane = lax.broadcasted_iota(jnp.int32, (lp, nx), 1)
    from_right = lane < nx // 2

    @pl.loop(0, n)
    def _(p):
        rows = pl.ds(pl.multiple_of(8 + p * lp, 8), lp)
        for c in range(3):
            for z in range(win):
                ext[c, z, rows, 0:nx] = own[p, c, z]
                ext[c, z, rows, nx : 2 * nx] = jnp.where(from_right, right[p, c, z], left[p, c, z])


def fill_from_halves(dims, ext, core, own, other):
    n, win, lp, nx = dims
    half = win - 2
    here = core[0]
    main = 3 * half * lp

    def place(source, p, c, w, z):
        at = c * half + w
        rows = pl.ds(pl.multiple_of(8 + p * lp, 8), lp)
        ext[c, z, rows, 0:nx] = source[p, pl.ds(pl.multiple_of(at * lp, 8), lp), :]
        for r in range(lp // 8):
            shift = 2 * nx - 2 - 4 * (r * 3 * half + at)
            part = pltpu.roll(source[p, main : main + 8, :], lax.rem(shift, nx), 1)
            ext[c, z, pl.ds(pl.multiple_of(8 + p * lp + 8 * r, 8), 8), nx : 2 * nx] = part

    @pl.loop(0, n)
    def _(p):
        for c in range(3):
            for w in range(half):
                place(own, p, c, w, w + 2 * here)
            for w in range(2):
                place(other, p, c, w + (half - 2) * here, w + half * (1 - here))


def column_kernel(dims, fill, sources, *refs):
    n, win, lp, nx = dims
    blocks, refs = refs[:sources], refs[sources:]
    weights, onehot, back, ext, bhi, blo, filt, lms, mms, whi, wlo = refs
    zs = win - 4
    ny = n * lp
    lanes = 2 * nx
    heavy = weights[...].astype(jnp.bfloat16)
    whi[...] = heavy
    wlo[...] = (weights[...] - heavy.astype(jnp.float32)).astype(jnp.bfloat16)

    zero = jnp.zeros((8, lanes), jnp.float32)
    for c in range(3):
        for z in range(win):
            ext[c, z, 0:8, :] = zero
            ext[c, z, ny + 8 : ny + 16, :] = zero
    fill(dims, ext, *blocks)

    @pl.loop(0, n)
    def _(p):
        base = pl.multiple_of(p * lp, 8)
        u = [[ext[c, z, pl.ds(base + 8, lp), :] for z in range(win)] for c in range(3)]
        boxes = [[None] * 21 for _ in range(zs)]
        for z in range(1, win - 1):
            v = [u[c][z] for c in range(3)]
            dx, dy, dz = [], [], []
            for c in range(3):
                dx.append(pltpu.roll(v[c], lanes - 1, 1) - pltpu.roll(v[c], 1, 1))
                tall = ext[c, z, pl.ds(base, lp + 16), :]
                dy.append(tall[9 : 9 + lp] - tall[7 : 7 + lp])
                dz.append(u[c][z + 1] - u[c][z - 1])
            s = strain_of(dx, dy, dz)
            mag = tensor_norm(s)
            fields = v + s + [v[i] * v[j] for i, j in PAIRS] + [mag * t for t in s]
            for o in range(zs):
                step = z - (o + 2)
                if -1 <= step <= 1:
                    for k in range(21):
                        term = fields[k] if step else 2.0 * fields[k]
                        boxes[o][k] = term if boxes[o][k] is None else boxes[o][k] + term
        for o in range(zs):
            for k in range(21):
                f = boxes[o][k]
                box = (pltpu.roll(f, 1, 1) + pltpu.roll(f, lanes - 1, 1) + 2.0 * f)[:, :nx] * 0.0625
                high = box.astype(jnp.bfloat16)
                cols = slice(o * nx, (o + 1) * nx)
                bhi[k, pl.ds(base, lp), cols] = high
                blo[k, pl.ds(base, lp), cols] = (box - high.astype(jnp.float32)).astype(jnp.bfloat16)

    @pl.loop(0, 21)
    def _(k):
        dot = functools.partial(jnp.dot, preferred_element_type=jnp.float32)
        filt[k] = dot(whi[...], bhi[k]) + (dot(whi[...], blo[k]) + dot(wlo[...], bhi[k]))

    @pl.loop(0, n)
    def _(p):
        base = pl.multiple_of(p * lp, 8)
        lm_total = jnp.zeros((lp, nx), jnp.float32)
        mm_total = jnp.zeros((lp, nx), jnp.float32)
        for o in range(zs):
            g = [filt[k, pl.ds(base, lp), o * nx : (o + 1) * nx] for k in range(21)]
            fmag = 4.0 * tensor_norm(g[3:9])
            for q, (i, j) in enumerate(PAIRS):
                leonard = g[9 + q] - g[i] * g[j]
                model = g[15 + q] - fmag * g[3 + q]
                weighted = model if q < 3 else 2.0 * model
                lm_total += leonard * weighted
                mm_total += model * weighted
                back[p, (q * zs + o) * lp : (q * zs + o + 1) * lp, :] = leonard
        lms[pl.ds(base, lp), :] = lm_total
        mms[pl.ds(base, lp), :] = mm_total

    ones = jnp.ones((8, nx), jnp.float32)
    exact = functools.partial(
        lax.dot_general, preferred_element_type=jnp.float32, precision=lax.Precision.HIGHEST
    )
    totals = []
    for part in (lms, mms):
        planes = exact(ones, part[...], (((1,), (1,)), ((), ())))
        totals.append(exact(planes, onehot[...], (((1,), (0,)), ((), ()))))
    row = lax.broadcasted_iota(jnp.int32, (8, onehot.shape[1]), 0)
    tile = jnp.where(row < 4, totals[0], totals[1])
    for p in range(n):
        back[p, 6 * zs * lp :, :] = tile


def magnitude_kernel(centre, right, left, below, above, out):
    _, lp, nz, nx = centre.shape
    lane = lax.broadcasted_iota(jnp.int32, (nz, nx), 1)
    for y in range(lp):
        v = [centre[c, y] for c in range(3)]
        dx, dy, dz = [], [], []
        for c in range(3):
            ahead = jnp.where(lane == nx - 1, pltpu.roll(right[c, y], nx - 1, 1), pltpu.roll(v[c], nx - 1, 1))
            behind = jnp.where(lane == 0, pltpu.roll(left[c, y], 1, 1), pltpu.roll(v[c], 1, 1))
            dx.append(ahead - behind)
            dz.append(pltpu.roll(v[c], nz - 1, 0) - pltpu.roll(v[c], 1, 0))
            up = centre[c, y + 1] if y + 1 < lp else above[c, 0]
            down = centre[c, y - 1] if y else below[c, 0]
            dy.append(up - down)
        out[y] = tensor_norm(strain_of(dx, dy, dz))


def local(velocity, filter_inverse, filter_block, plane_bin):
    _, lp, nz, nx = velocity.shape
    n = lax.axis_size("pz")
    m = lax.axis_size("px")
    ny, zs = n * lp, nz // n
    win = zs + 4
    half = zs + 2
    shared = m == 2 and n % 2 == 0 and 12 * half * (lp // 8) <= nx
    swap = [(0, 1), (1, 0)]
    core = lax.axis_index("px")

    same = (filter_block[:, None] == filter_block[None, :]).astype(jnp.float32)
    masked = filter_inverse * same
    weights = masked / jnp.sum(masked, axis=1, keepdims=True)
    onehot = (plane_bin[:, None] == jnp.arange(nx, dtype=jnp.int32)[None, :]).astype(jnp.float32)

    right = lax.ppermute(velocity, "px", [((i + 1) % m, i) for i in range(m)])
    left = right if m == 2 else lax.ppermute(velocity, "px", [(i, (i + 1) % m) for i in range(m)])
    below = lax.ppermute(velocity[:, -1:], "pz", [(i, i + 1) for i in range(n - 1)])
    above = lax.ppermute(velocity[:, :1], "pz", [(i + 1, i) for i in range(n - 1)])
    magnitude = pl.pallas_call(
        magnitude_kernel,
        out_shape=jax.ShapeDtypeStruct((lp, nz, nx), jnp.float32),
        cost_estimate=pl.CostEstimate(flops=60 * lp * nz * nx, bytes_accessed=40 * lp * nz * nx, transcendentals=0),
    )(velocity, right, left, below, above)

    if shared:
        zg = 2 * zs
        chunks, edges = [], []
        halves = [jnp.where(core == h, velocity, right) for h in range(2)]
        for h in range(2):
            outer = halves[1 - h]
            edge = jnp.concatenate([outer[..., -2:], outer[..., :2]], axis=3)
            for part, dest in ((halves[h], chunks), (edge, edges)):
                turned = jnp.transpose(part, (0, 2, 1, 3))
                turned = jnp.concatenate([turned[:, -2:], turned, turned[:, :2]], axis=1)
                turned = lax.dynamic_slice_in_dim(turned, core * half, nz - zg + half, 1)
                dest.append(jnp.stack([turned[:, g * zg : g * zg + half] for g in range(n // 2)]))
        main = jnp.stack(chunks, axis=1).reshape(n, 3 * half * lp, nx)
        edge = jnp.stack(edges, axis=1).reshape(n, 3, half, lp // 8, 8, 4)
        edge = jnp.transpose(edge, (0, 4, 3, 1, 2, 5)).reshape(n, 8, 12 * half * (lp // 8))
        edge = jnp.pad(edge, ((0, 0), (0, 0), (0, nx - edge.shape[2])))
        sent = jnp.concatenate([main, edge], axis=1)
        own = lax.all_to_all(sent, "pz", split_axis=0, concat_axis=0, tiled=True)
        other = lax.ppermute(own, "px", swap)
        fill, blocks = fill_from_halves, (core.astype(jnp.int32).reshape(1), own, other)
        specs = [pl.BlockSpec(memory_space=pltpu.SMEM)] + [pl.BlockSpec(memory_space=pltpu.VMEM)] * 2
    else:
        turned = jnp.transpose(velocity, (0, 2, 1, 3))
        turned = jnp.concatenate([turned[:, -2:], turned, turned[:, :2]], axis=1)
        sent = jnp.stack([turned[:, t * zs : t * zs + win] for t in range(n)])
        own = lax.all_to_all(sent, "pz", split_axis=0, concat_axis=0, tiled=True)
        ahead = lax.ppermute(own, "px", [((i + 1) % m, i) for i in range(m)])
        behind = lax.ppermute(own, "px", [(i, (i + 1) % m) for i in range(m)])
        fill, blocks = fill_from_blocks, (own, ahead, behind)
        specs = [pl.BlockSpec(memory_space=pltpu.VMEM)] * 3

    rows = 6 * zs * lp
    back = pl.pallas_call(
        functools.partial(column_kernel, (n, win, lp, nx), fill, len(blocks)),
        out_shape=jax.ShapeDtypeStruct((n, rows + 8, nx), jnp.float32),
        in_specs=specs + [pl.BlockSpec(memory_space=pltpu.VMEM)] * 2,
        out_specs=pl.BlockSpec(memory_space=pltpu.VMEM),
        scratch_shapes=[
            pltpu.VMEM((3, win, ny + 16, 2 * nx), jnp.float32),
            pltpu.VMEM((21, ny, zs * nx), jnp.bfloat16),
            pltpu.VMEM((21, ny, zs * nx), jnp.bfloat16),
            pltpu.VMEM((21, ny, zs * nx), jnp.float32),
            pltpu.VMEM((ny, nx), jnp.float32),
            pltpu.VMEM((ny, nx), jnp.float32),
            pltpu.VMEM((ny, ny), jnp.bfloat16),
            pltpu.VMEM((ny, ny), jnp.bfloat16),
        ],
        compiler_params=pltpu.CompilerParams(vmem_limit_bytes=60 * 1024 * 1024),
    )(*blocks, weights, onehot)

    home = lax.all_to_all(back, "pz", split_axis=0, concat_axis=0, tiled=True)
    totals = jnp.sum(home[:, rows:], axis=0)
    stress = home[:, :rows]
    if shared:
        totals = totals + lax.ppermute(totals, "px", swap)
        stress = stress.reshape(n // 2, 2, 6, zs, lp, nx)
        mine = lax.dynamic_index_in_dim(stress, core, 1, keepdims=False)
        give = lax.dynamic_index_in_dim(stress, 1 - core, 1, keepdims=False)
        got = lax.ppermute(give, "px", swap)
        first, second = jnp.where(core == 0, mine, got), jnp.where(core == 0, got, mine)
        stress = jnp.stack([first, second], axis=1)
        leonard = jnp.transpose(stress, (2, 4, 0, 1, 3, 5)).reshape(6, lp, nz, nx)
    else:
        totals = lax.psum(totals, "px")
        stress = stress.reshape(n, 6, zs, lp, nx)
        leonard = jnp.transpose(stress, (1, 3, 0, 2, 4)).reshape(6, lp, nz, nx)
    numer, denom = totals[0, :NBIN], totals[4, :NBIN]
    cells = nx * m * nz
    per_bin = numer / jnp.maximum(denom, jnp.float32(cells))
    coefficient = jnp.dot(onehot[:, :NBIN], per_bin, precision=lax.Precision.HIGHEST)
    local_coef = lax.dynamic_slice_in_dim(coefficient, lax.axis_index("pz") * lp, lp, 0)
    viscosity = local_coef[:, None, None] * magnitude
    return (leonard, viscosity, coefficient)


def solution(mesh):
    return jax.shard_map(
        local,
        mesh=mesh,
        in_specs=(P(None, "pz", None, "px"), P(), P(), P()),
        out_specs=(P(None, "pz", None, "px"), P("pz", None, "px"), P()),
        check_vma=False,
    )
```

```python
import functools

import jax
import jax.numpy as jnp
from jax import lax
from jax.experimental import pallas as pl
from jax.experimental.pallas import tpu as pltpu
from jax.sharding import PartitionSpec as P

NBIN = 64
MESH = pl.DeviceIdType.MESH
PAIRS = ((0, 0), (1, 1), (2, 2), (0, 1), (0, 2), (1, 2))


def tensor_norm(s):
    diag = s[0] * s[0] + s[1] * s[1] + s[2] * s[2]
    off = s[3] * s[3] + s[4] * s[4] + s[5] * s[5]
    return jnp.sqrt(2.0 * diag + 4.0 * off)


def strain_of(dx, dy, dz):
    return [
        dx[0] * 0.5,
        dy[1] * 0.5,
        dz[2] * 0.5,
        0.25 * (dy[0] + dx[1]),
        0.25 * (dz[0] + dx[2]),
        0.25 * (dz[1] + dy[2]),
    ]


def fill_from_blocks(dims, ext, own, right, left):
    n, win, lp, nx = dims
    lane = lax.broadcasted_iota(jnp.int32, (lp, nx), 1)
    from_right = lane < nx // 2

    @pl.loop(0, n)
    def _(p):
        rows = pl.ds(pl.multiple_of(8 + p * lp, 8), lp)
        for c in range(3):
            for z in range(win):
                ext[c, z, rows, 0:nx] = own[p, c, z]
                ext[c, z, rows, nx : 2 * nx] = jnp.where(from_right, right[p, c, z], left[p, c, z])


def fill_from_halves(dims, ext, core, own, other):
    n, win, lp, nx = dims
    half = win - 2
    here = core[0]

    def place(source, main, p, c, w, at, z):
        rows = pl.ds(pl.multiple_of(8 + p * lp, 8), lp)
        ext[c, z, rows, 0:nx] = source[p, (w * 3 + c) * lp : (w * 3 + c + 1) * lp, :]
        for r in range(lp // 8):
            shift = 2 * nx - 2 - 4 * (r * 3 * half + at)
            part = pltpu.roll(source[p, main : main + 8, :], lax.rem(shift, nx), 1)
            ext[c, z, pl.ds(pl.multiple_of(8 + p * lp + 8 * r, 8), 8), nx : 2 * nx] = part

    @pl.loop(0, n)
    def _(p):
        for c in range(3):
            for w in range(half):
                place(own, 3 * half * lp, p, c, w, w * 3 + c, w + 2 * here)
            for w in range(2):
                at = (w + (half - 2) * here) * 3 + c
                place(other, 6 * lp, p, c, w, at, w + half * (1 - here))


def column_kernel(dims, fill, sources, *refs):
    n, win, lp, nx = dims
    blocks, refs = refs[:sources], refs[sources:]
    weights, onehot, back, ext, bhi, blo, filt, lms, mms, whi, wlo = refs
    zs = win - 4
    ny = n * lp
    lanes = 2 * nx
    heavy = weights[...].astype(jnp.bfloat16)
    whi[...] = heavy
    wlo[...] = (weights[...] - heavy.astype(jnp.float32)).astype(jnp.bfloat16)

    zero = jnp.zeros((8, lanes), jnp.float32)
    for c in range(3):
        for z in range(win):
            ext[c, z, 0:8, :] = zero
            ext[c, z, ny + 8 : ny + 16, :] = zero
    fill(dims, ext, *blocks)

    @pl.loop(0, n)
    def _(p):
        base = pl.multiple_of(p * lp, 8)
        u = [[ext[c, z, pl.ds(base + 8, lp), :] for z in range(win)] for c in range(3)]
        boxes = [[None] * 21 for _ in range(zs)]
        for z in range(1, win - 1):
            v = [u[c][z] for c in range(3)]
            dx, dy, dz = [], [], []
            for c in range(3):
                dx.append(pltpu.roll(v[c], lanes - 1, 1) - pltpu.roll(v[c], 1, 1))
                tall = ext[c, z, pl.ds(base, lp + 16), :]
                dy.append(tall[9 : 9 + lp] - tall[7 : 7 + lp])
                dz.append(u[c][z + 1] - u[c][z - 1])
            s = strain_of(dx, dy, dz)
            mag = tensor_norm(s)
            fields = v + s + [v[i] * v[j] for i, j in PAIRS] + [mag * t for t in s]
            for o in range(zs):
                step = z - (o + 2)
                if -1 <= step <= 1:
                    for k in range(21):
                        term = fields[k] if step else 2.0 * fields[k]
                        boxes[o][k] = term if boxes[o][k] is None else boxes[o][k] + term
        for o in range(zs):
            for k in range(21):
                f = boxes[o][k]
                box = (pltpu.roll(f, 1, 1) + pltpu.roll(f, lanes - 1, 1) + 2.0 * f)[:, :nx] * 0.0625
                high = box.astype(jnp.bfloat16)
                cols = slice(o * nx, (o + 1) * nx)
                bhi[k, pl.ds(base, lp), cols] = high
                blo[k, pl.ds(base, lp), cols] = (box - high.astype(jnp.float32)).astype(jnp.bfloat16)

    @pl.loop(0, 21)
    def _(k):
        dot = functools.partial(jnp.dot, preferred_element_type=jnp.float32)
        filt[k] = dot(whi[...], bhi[k]) + (dot(whi[...], blo[k]) + dot(wlo[...], bhi[k]))

    @pl.loop(0, n)
    def _(p):
        base = pl.multiple_of(p * lp, 8)
        lm_total = jnp.zeros((lp, nx), jnp.float32)
        mm_total = jnp.zeros((lp, nx), jnp.float32)
        for o in range(zs):
            g = [filt[k, pl.ds(base, lp), o * nx : (o + 1) * nx] for k in range(21)]
            fmag = 4.0 * tensor_norm(g[3:9])
            for q, (i, j) in enumerate(PAIRS):
                leonard = g[9 + q] - g[i] * g[j]
                model = g[15 + q] - fmag * g[3 + q]
                weighted = model if q < 3 else 2.0 * model
                lm_total += leonard * weighted
                mm_total += model * weighted
                back[p, (q * zs + o) * lp : (q * zs + o + 1) * lp, :] = leonard
        lms[pl.ds(base, lp), :] = lm_total
        mms[pl.ds(base, lp), :] = mm_total

    ones = jnp.ones((8, nx), jnp.float32)
    exact = functools.partial(
        lax.dot_general, preferred_element_type=jnp.float32, precision=lax.Precision.HIGHEST
    )
    totals = []
    for part in (lms, mms):
        planes = exact(ones, part[...], (((1,), (1,)), ((), ())))
        totals.append(exact(planes, onehot[...], (((1,), (0,)), ((), ()))))
    row = lax.broadcasted_iota(jnp.int32, (8, onehot.shape[1]), 0)
    tile = jnp.where(row < 4, totals[0], totals[1])
    for p in range(n):
        back[p, 6 * zs * lp :, :] = tile


def greet_all(m, n):
    me = lax.axis_index("px") * n + lax.axis_index("pz")
    barrier = pltpu.get_barrier_semaphore()

    @pl.loop(1, m * n)
    def _(step):
        peer = lax.rem(me + step, m * n)
        pl.semaphore_signal(barrier, inc=1, device_id=(peer // n, lax.rem(peer, n)), device_id_type=MESH)

    pl.semaphore_wait(barrier, m * n - 1)


def outward_kernel(dims, main, edge, own, other, main_out, main_in, edge_out, edge_in, pass_out, pass_in):
    n, half, lp = dims
    a, s = lax.axis_index("px"), lax.axis_index("pz")
    rows = 3 * half * lp
    greet_all(2, n)

    def send(source, t, parity, dst, out_sem, in_sem):
        core, chip = lax.rem(t, 2), 2 * (t // 2) + parity
        itself = (core == a) & (chip == s)
        copy = pltpu.make_async_remote_copy(
            source.at[t], dst, out_sem.at[t], in_sem.at[s], device_id=(core, chip), device_id_type=MESH
        )
        return itself, copy, pltpu.make_async_copy(source.at[t], dst, in_sem.at[s])

    def sends(t):
        return (
            send(edge, t, 1 - a, own.at[s, rows : rows + 8], edge_out, edge_in),
            send(main, t, a, own.at[s, 0:rows], main_out, main_in),
        )

    @pl.loop(0, n)
    def _(i):
        for itself, copy, here in sends(lax.rem(s + i, n)):
            pl.when(itself)(here.start)
            pl.when(jnp.logical_not(itself))(copy.start)

    first = (1 - a) * (half - 2) * 3 * lp

    def passes(p):
        return [
            pltpu.make_async_remote_copy(
                own.at[p, src], other.at[p, dst], pass_out.at[j, p], pass_in.at[j, p],
                device_id=(1 - a, s), device_id_type=MESH,
            )
            for j, (src, dst) in enumerate(
                (
                    (pl.ds(pl.multiple_of(first, 8), 6 * lp), slice(0, 6 * lp)),
                    (slice(rows, rows + 8), slice(6 * lp, 6 * lp + 8)),
                )
            )
        ]

    @pl.loop(0, n)
    def _(i):
        p = lax.rem(s + n - i, n)
        pltpu.make_async_copy(main.at[0], own.at[p, 0:rows], main_in.at[p]).wait()
        pltpu.make_async_copy(edge.at[0], own.at[p, rows : rows + 8], edge_in.at[p]).wait()
        for copy in passes(p):
            copy.start()

    @pl.loop(0, n)
    def _(p):
        for copy in passes(p):
            copy.wait()
        for itself, copy, here in sends(p):
            pl.when(jnp.logical_not(itself))(copy.wait_send)


def return_kernel(n, back, velocity, home, out, beside, near, back_out, back_in, halo_out, halo_in):
    _, lp, nz, nx = velocity.shape
    a, s = lax.axis_index("px"), lax.axis_index("pz")
    greet_all(2, n)
    slot = 2 * (s // 2) + a
    parity = lax.rem(s, 2)
    remote = functools.partial(pltpu.make_async_remote_copy, device_id_type=MESH)
    halos = [
        remote(velocity, beside, halo_out.at[0], halo_in.at[0], device_id=(1 - a, s)),
        remote(velocity.at[:, lp - 1], near.at[0], halo_out.at[1], halo_in.at[1], device_id=(a, lax.rem(s + 1, n))),
        remote(velocity.at[:, 0], near.at[1], halo_out.at[2], halo_in.at[2], device_id=(a, lax.rem(s + n - 1, n))),
    ]
    for copy in halos:
        copy.start()

    def send(p):
        itself = (parity == a) & (p == s)
        copy = remote(back.at[p], home.at[slot], back_out.at[p], back_in.at[slot], device_id=(parity, p))
        return itself, copy, pltpu.make_async_copy(back.at[p], home.at[slot], back_in.at[slot])

    @pl.loop(0, n)
    def _(i):
        itself, copy, here = send(lax.rem(s + i, n))
        pl.when(itself)(here.start)
        pl.when(jnp.logical_not(itself))(copy.start)

    for copy in halos:
        copy.wait()
    lane = lax.broadcasted_iota(jnp.int32, (nz, nx), 1)
    has_below = (s > 0).astype(jnp.float32)
    has_above = (s < n - 1).astype(jnp.float32)

    def plane(y, ups, downs):
        dx, dy, dz = [], [], []
        for c in range(3):
            v, side = velocity[c, y], beside[c, y]
            ahead = jnp.where(lane == nx - 1, pltpu.roll(side, nx - 1, 1), pltpu.roll(v, nx - 1, 1))
            behind = jnp.where(lane == 0, pltpu.roll(side, 1, 1), pltpu.roll(v, 1, 1))
            dx.append(ahead - behind)
            dz.append(pltpu.roll(v, nz - 1, 0) - pltpu.roll(v, 1, 0))
            dy.append(ups[c] - downs[c])
        out[y] = tensor_norm(strain_of(dx, dy, dz))

    line = [near[0, c] * has_below for c in range(3)]
    plane(0, [velocity[c, 1] for c in range(3)], line)
    line = [near[1, c] * has_above for c in range(3)]
    plane(lp - 1, line, [velocity[c, lp - 2] for c in range(3)])

    @pl.loop(1, lp - 1)
    def _(y):
        plane(y, [velocity[c, y + 1] for c in range(3)], [velocity[c, y - 1] for c in range(3)])

    @pl.loop(0, n)
    def _(p):
        pltpu.make_async_copy(back.at[0], home.at[p], back_in.at[p]).wait()
        itself, copy, here = send(p)
        pl.when(jnp.logical_not(itself))(copy.wait_send)


def magnitude_kernel(centre, right, left, below, above, out):
    _, lp, nz, nx = centre.shape
    lane = lax.broadcasted_iota(jnp.int32, (nz, nx), 1)
    for y in range(lp):
        v = [centre[c, y] for c in range(3)]
        dx, dy, dz = [], [], []
        for c in range(3):
            ahead = jnp.where(lane == nx - 1, pltpu.roll(right[c, y], nx - 1, 1), pltpu.roll(v[c], nx - 1, 1))
            behind = jnp.where(lane == 0, pltpu.roll(left[c, y], 1, 1), pltpu.roll(v[c], 1, 1))
            dx.append(ahead - behind)
            dz.append(pltpu.roll(v[c], nz - 1, 0) - pltpu.roll(v[c], 1, 0))
            up = centre[c, y + 1] if y + 1 < lp else above[c, 0]
            down = centre[c, y - 1] if y else below[c, 0]
            dy.append(up - down)
        out[y] = tensor_norm(strain_of(dx, dy, dz))


def local(velocity, filter_inverse, filter_block, plane_bin):
    _, lp, nz, nx = velocity.shape
    n = lax.axis_size("pz")
    m = lax.axis_size("px")
    ny, zs = n * lp, nz // n
    win = zs + 4
    half = zs + 2
    shared = m == 2 and n % 2 == 0 and 12 * half * (lp // 8) <= nx
    core = lax.axis_index("px")

    same = (filter_block[:, None] == filter_block[None, :]).astype(jnp.float32)
    masked = filter_inverse * same
    weights = masked / jnp.sum(masked, axis=1, keepdims=True)
    onehot = (plane_bin[:, None] == jnp.arange(nx, dtype=jnp.int32)[None, :]).astype(jnp.float32)

    if shared:
        zg = 2 * zs
        chunks = []
        for part in (velocity, jnp.concatenate([velocity[..., -2:], velocity[..., :2]], axis=3)):
            turned = jnp.transpose(part, (2, 0, 1, 3))
            turned = jnp.concatenate([turned[-2:], turned, turned[:2]], axis=0)
            starts = [(t // 2) * zg + (t % 2) * half for t in range(n)]
            chunks.append(jnp.stack([turned[i : i + half] for i in starts]))
        main = chunks[0].reshape(n, 3 * half * lp, nx)
        edge = chunks[1].reshape(n, half * 3, lp // 8, 8, 4)
        edge = jnp.transpose(edge, (0, 3, 2, 1, 4)).reshape(n, 8, 12 * half * (lp // 8))
        edge = jnp.pad(edge, ((0, 0), (0, 0), (0, nx - edge.shape[2])))
        own, other = pl.pallas_call(
            functools.partial(outward_kernel, (n, half, lp)),
            out_shape=(
                jax.ShapeDtypeStruct((n, 3 * half * lp + 8, nx), jnp.float32),
                jax.ShapeDtypeStruct((n, 6 * lp + 8, nx), jnp.float32),
            ),
            in_specs=[pl.BlockSpec(memory_space=pltpu.VMEM)] * 2,
            out_specs=(pl.BlockSpec(memory_space=pltpu.VMEM),) * 2,
            scratch_shapes=[pltpu.SemaphoreType.DMA((n,))] * 4 + [pltpu.SemaphoreType.DMA((2, n))] * 2,
            compiler_params=pltpu.CompilerParams(collective_id=0, has_side_effects=True),
        )(main, edge)
        fill, blocks = fill_from_halves, (core.astype(jnp.int32).reshape(1), own, other)
        specs = [pl.BlockSpec(memory_space=pltpu.SMEM)] + [pl.BlockSpec(memory_space=pltpu.VMEM)] * 2
    else:
        right = lax.ppermute(velocity, "px", [((i + 1) % m, i) for i in range(m)])
        left = right if m == 2 else lax.ppermute(velocity, "px", [(i, (i + 1) % m) for i in range(m)])
        below = lax.ppermute(velocity[:, -1:], "pz", [(i, i + 1) for i in range(n - 1)])
        above = lax.ppermute(velocity[:, :1], "pz", [(i + 1, i) for i in range(n - 1)])
        magnitude = pl.pallas_call(
            magnitude_kernel,
            out_shape=jax.ShapeDtypeStruct((lp, nz, nx), jnp.float32),
            cost_estimate=pl.CostEstimate(flops=60 * lp * nz * nx, bytes_accessed=40 * lp * nz * nx, transcendentals=0),
        )(velocity, right, left, below, above)
        turned = jnp.transpose(velocity, (0, 2, 1, 3))
        turned = jnp.concatenate([turned[:, -2:], turned, turned[:, :2]], axis=1)
        sent = jnp.stack([turned[:, t * zs : t * zs + win] for t in range(n)])
        own = lax.all_to_all(sent, "pz", split_axis=0, concat_axis=0, tiled=True)
        ahead = lax.ppermute(own, "px", [((i + 1) % m, i) for i in range(m)])
        behind = lax.ppermute(own, "px", [(i, (i + 1) % m) for i in range(m)])
        fill, blocks = fill_from_blocks, (own, ahead, behind)
        specs = [pl.BlockSpec(memory_space=pltpu.VMEM)] * 3

    rows = 6 * zs * lp
    back = pl.pallas_call(
        functools.partial(column_kernel, (n, win, lp, nx), fill, len(blocks)),
        out_shape=jax.ShapeDtypeStruct((n, rows + 8, nx), jnp.float32),
        in_specs=specs + [pl.BlockSpec(memory_space=pltpu.VMEM)] * 2,
        out_specs=pl.BlockSpec(memory_space=pltpu.VMEM),
        scratch_shapes=[
            pltpu.VMEM((3, win, ny + 16, 2 * nx), jnp.float32),
            pltpu.VMEM((21, ny, zs * nx), jnp.bfloat16),
            pltpu.VMEM((21, ny, zs * nx), jnp.bfloat16),
            pltpu.VMEM((21, ny, zs * nx), jnp.float32),
            pltpu.VMEM((ny, nx), jnp.float32),
            pltpu.VMEM((ny, nx), jnp.float32),
            pltpu.VMEM((ny, ny), jnp.bfloat16),
            pltpu.VMEM((ny, ny), jnp.bfloat16),
        ],
        compiler_params=pltpu.CompilerParams(vmem_limit_bytes=60 * 1024 * 1024),
    )(*blocks, weights, onehot)

    if shared:
        home, magnitude = pl.pallas_call(
            functools.partial(return_kernel, n),
            out_shape=(
                jax.ShapeDtypeStruct(back.shape, jnp.float32),
                jax.ShapeDtypeStruct((lp, nz, nx), jnp.float32),
            ),
            in_specs=[pl.BlockSpec(memory_space=pltpu.VMEM)] * 2,
            out_specs=(pl.BlockSpec(memory_space=pltpu.VMEM),) * 2,
            scratch_shapes=[
                pltpu.VMEM((3, lp, nz, nx), jnp.float32),
                pltpu.VMEM((2, 3, nz, nx), jnp.float32),
                pltpu.SemaphoreType.DMA((n,)),
                pltpu.SemaphoreType.DMA((n,)),
                pltpu.SemaphoreType.DMA((3,)),
                pltpu.SemaphoreType.DMA((3,)),
            ],
            compiler_params=pltpu.CompilerParams(collective_id=1, has_side_effects=True),
        )(back, velocity)
        totals = jnp.sum(home[:, rows:], axis=0)
        totals = totals + lax.ppermute(totals, "px", [(0, 1), (1, 0)])
    else:
        home = lax.all_to_all(back, "pz", split_axis=0, concat_axis=0, tiled=True)
        totals = lax.psum(jnp.sum(home[:, rows:], axis=0), "px")
    stress = home[:, :rows].reshape(n, 6, zs, lp, nx)
    leonard = jnp.transpose(stress, (1, 3, 0, 2, 4)).reshape(6, lp, nz, nx)
    numer, denom = totals[0, :NBIN], totals[4, :NBIN]
    cells = nx * m * nz
    per_bin = numer / jnp.maximum(denom, jnp.float32(cells))
    coefficient = jnp.dot(onehot[:, :NBIN], per_bin, precision=lax.Precision.HIGHEST)
    local_coef = lax.dynamic_slice_in_dim(coefficient, lax.axis_index("pz") * lp, lp, 0)
    viscosity = local_coef[:, None, None] * magnitude
    return (leonard, viscosity, coefficient)


def solution(mesh):
    return jax.shard_map(
        local,
        mesh=mesh,
        in_specs=(P(None, "pz", None, "px"), P(), P(), P()),
        out_specs=(P(None, "pz", None, "px"), P("pz", None, "px"), P()),
        check_vma=False,
    )
```

```python
import functools

import jax
import jax.numpy as jnp
from jax import lax
from jax.experimental import pallas as pl
from jax.experimental.pallas import tpu as pltpu
from jax.sharding import PartitionSpec as P

NBIN = 64
MESH = pl.DeviceIdType.MESH
PAIRS = ((0, 0), (1, 1), (2, 2), (0, 1), (0, 2), (1, 2))


def tensor_norm(s):
    diag = s[0] * s[0] + s[1] * s[1] + s[2] * s[2]
    off = s[3] * s[3] + s[4] * s[4] + s[5] * s[5]
    return jnp.sqrt(2.0 * diag + 4.0 * off)


def strain_of(dx, dy, dz):
    return [
        dx[0] * 0.5,
        dy[1] * 0.5,
        dz[2] * 0.5,
        0.25 * (dy[0] + dx[1]),
        0.25 * (dz[0] + dx[2]),
        0.25 * (dz[1] + dy[2]),
    ]


def fill_from_blocks(dims, ext, own, right, left):
    n, win, lp, nx = dims
    lane = lax.broadcasted_iota(jnp.int32, (lp, nx), 1)
    from_right = lane < nx // 2

    @pl.loop(0, n)
    def _(p):
        rows = pl.ds(pl.multiple_of(8 + p * lp, 8), lp)
        for c in range(3):
            for z in range(win):
                ext[c, z, rows, 0:nx] = own[p, c, z]
                ext[c, z, rows, nx : 2 * nx] = jnp.where(from_right, right[p, c, z], left[p, c, z])


def fill_from_halves(dims, ext, core, own, own_edge, other, other_edge):
    n, win, lp, nx = dims
    half = win - 2
    here = core[0]

    def place(source, edges, p, c, w, at, z):
        rows = pl.ds(pl.multiple_of(8 + p * lp, 8), lp)
        ext[c, z, rows, 0:nx] = source[p, w, c * lp : (c + 1) * lp, :]
        for r in range(lp // 8):
            shift = 2 * nx - 2 - 4 * (r * 3 * half + at)
            part = pltpu.roll(edges[p], lax.rem(shift, nx), 1)
            ext[c, z, pl.ds(pl.multiple_of(8 + p * lp + 8 * r, 8), 8), nx : 2 * nx] = part

    @pl.loop(0, n)
    def _(p):
        for c in range(3):
            for w in range(half):
                place(own, own_edge, p, c, w, w * 3 + c, w + 2 * here)
            for w in range(2):
                at = (w + (half - 2) * here) * 3 + c
                place(other, other_edge, p, c, w, at, w + half * (1 - here))


def column_kernel(dims, fill, sources, *refs):
    n, win, lp, nx = dims
    blocks, refs = refs[:sources], refs[sources:]
    weights, onehot, back, ext, bhi, blo, filt, lms, mms, whi, wlo = refs
    zs = win - 4
    ny = n * lp
    lanes = 2 * nx
    heavy = weights[...].astype(jnp.bfloat16)
    whi[...] = heavy
    wlo[...] = (weights[...] - heavy.astype(jnp.float32)).astype(jnp.bfloat16)

    zero = jnp.zeros((8, lanes), jnp.float32)
    for c in range(3):
        for z in range(win):
            ext[c, z, 0:8, :] = zero
            ext[c, z, ny + 8 : ny + 16, :] = zero
    fill(dims, ext, *blocks)

    @pl.loop(0, n)
    def _(p):
        base = pl.multiple_of(p * lp, 8)
        u = [[ext[c, z, pl.ds(base + 8, lp), :] for z in range(win)] for c in range(3)]
        boxes = [[None] * 21 for _ in range(zs)]
        for z in range(1, win - 1):
            v = [u[c][z] for c in range(3)]
            dx, dy, dz = [], [], []
            for c in range(3):
                dx.append(pltpu.roll(v[c], lanes - 1, 1) - pltpu.roll(v[c], 1, 1))
                tall = ext[c, z, pl.ds(base, lp + 16), :]
                dy.append(tall[9 : 9 + lp] - tall[7 : 7 + lp])
                dz.append(u[c][z + 1] - u[c][z - 1])
            s = strain_of(dx, dy, dz)
            mag = tensor_norm(s)
            fields = v + s + [v[i] * v[j] for i, j in PAIRS] + [mag * t for t in s]
            for o in range(zs):
                step = z - (o + 2)
                if -1 <= step <= 1:
                    for k in range(21):
                        term = fields[k] if step else 2.0 * fields[k]
                        boxes[o][k] = term if boxes[o][k] is None else boxes[o][k] + term
        for o in range(zs):
            for k in range(21):
                f = boxes[o][k]
                box = (pltpu.roll(f, 1, 1) + pltpu.roll(f, lanes - 1, 1) + 2.0 * f)[:, :nx] * 0.0625
                high = box.astype(jnp.bfloat16)
                cols = slice(o * nx, (o + 1) * nx)
                bhi[k, pl.ds(base, lp), cols] = high
                blo[k, pl.ds(base, lp), cols] = (box - high.astype(jnp.float32)).astype(jnp.bfloat16)

    @pl.loop(0, 21)
    def _(k):
        dot = functools.partial(jnp.dot, preferred_element_type=jnp.float32)
        filt[k] = dot(whi[...], bhi[k]) + (dot(whi[...], blo[k]) + dot(wlo[...], bhi[k]))

    @pl.loop(0, n)
    def _(p):
        base = pl.multiple_of(p * lp, 8)
        lm_total = jnp.zeros((lp, nx), jnp.float32)
        mm_total = jnp.zeros((lp, nx), jnp.float32)
        for o in range(zs):
            g = [filt[k, pl.ds(base, lp), o * nx : (o + 1) * nx] for k in range(21)]
            fmag = 4.0 * tensor_norm(g[3:9])
            for q, (i, j) in enumerate(PAIRS):
                leonard = g[9 + q] - g[i] * g[j]
                model = g[15 + q] - fmag * g[3 + q]
                weighted = model if q < 3 else 2.0 * model
                lm_total += leonard * weighted
                mm_total += model * weighted
                back[p, (q * zs + o) * lp : (q * zs + o + 1) * lp, :] = leonard
        lms[pl.ds(base, lp), :] = lm_total
        mms[pl.ds(base, lp), :] = mm_total

    ones = jnp.ones((8, nx), jnp.float32)
    exact = functools.partial(
        lax.dot_general, preferred_element_type=jnp.float32, precision=lax.Precision.HIGHEST
    )
    totals = []
    for part in (lms, mms):
        planes = exact(ones, part[...], (((1,), (1,)), ((), ())))
        totals.append(exact(planes, onehot[...], (((1,), (0,)), ((), ()))))
    row = lax.broadcasted_iota(jnp.int32, (8, onehot.shape[1]), 0)
    tile = jnp.where(row < 4, totals[0], totals[1])
    for p in range(n):
        back[p, 6 * zs * lp :, :] = tile


def greet_all(m, n):
    me = lax.axis_index("px") * n + lax.axis_index("pz")
    barrier = pltpu.get_barrier_semaphore()

    @pl.loop(1, m * n)
    def _(step):
        peer = lax.rem(me + step, m * n)
        pl.semaphore_signal(barrier, inc=1, device_id=(peer // n, lax.rem(peer, n)), device_id_type=MESH)

    pl.semaphore_wait(barrier, m * n - 1)


def edge_kernel(dims, main, edge):
    half, lp, nx = dims
    lane = lax.broadcasted_iota(jnp.int32, (8, nx), 1)

    @pl.loop(0, edge.shape[0])
    def _(i):
        tile = jnp.zeros((8, nx), jnp.float32)
        for r in range(lp // 8):
            for w in range(half):
                for c in range(3):
                    at = 4 * ((r * half + w) * 3 + c)
                    cells = main[i * half + w, c * lp + r * 8 : c * lp + r * 8 + 8, :]
                    tile = jnp.where((lane >= at) & (lane < at + 4), pltpu.roll(cells, (at + 2) % nx, 1), tile)
        edge[i] = tile


def outward_kernel(dims, main, edge, own, own_edge, other, other_edge, main_out, main_in, edge_out, edge_in, pass_out, pass_in):
    n, half, lp = dims
    a, s = lax.axis_index("px"), lax.axis_index("pz")
    greet_all(2, n)

    def send(source, t, parity, dst, out_sem, in_sem):
        core, chip = lax.rem(t, 2), 2 * (t // 2) + parity
        itself = (core == a) & (chip == s)
        copy = pltpu.make_async_remote_copy(
            source, dst, out_sem.at[t], in_sem.at[s], device_id=(core, chip), device_id_type=MESH
        )
        return itself, copy, pltpu.make_async_copy(source, dst, in_sem.at[s])

    def sends(t):
        return (
            send(edge.at[t // 2 + lax.rem(t, 2)], t, 1 - a, own_edge.at[s], edge_out, edge_in),
            send(main.at[pl.ds((t // 2 + lax.rem(t, 2)) * half, half)], t, a, own.at[s], main_out, main_in),
        )

    @pl.loop(0, n)
    def _(i):
        for itself, copy, here in sends(lax.rem(s + i, n)):
            pl.when(itself)(here.start)
            pl.when(jnp.logical_not(itself))(copy.start)

    first = (1 - a) * (half - 2)

    def passes(p):
        return [
            pltpu.make_async_remote_copy(
                src, dst, pass_out.at[j, p], pass_in.at[j, p],
                device_id=(1 - a, s), device_id_type=MESH,
            )
            for j, (src, dst) in enumerate(
                ((own.at[p, pl.ds(first, 2)], other.at[p]), (own_edge.at[p], other_edge.at[p]))
            )
        ]

    @pl.loop(0, n)
    def _(i):
        p = lax.rem(s + n - i, n)
        pltpu.make_async_copy(main.at[0:half], own.at[p], main_in.at[p]).wait()
        pltpu.make_async_copy(edge.at[0], own_edge.at[p], edge_in.at[p]).wait()
        for copy in passes(p):
            copy.start()

    @pl.loop(0, n)
    def _(p):
        for copy in passes(p):
            copy.wait()
        for itself, copy, here in sends(p):
            pl.when(jnp.logical_not(itself))(copy.wait_send)


def return_kernel(n, back, velocity, home, out, beside, near, back_out, back_in, halo_out, halo_in):
    _, lp, nz, nx = velocity.shape
    a, s = lax.axis_index("px"), lax.axis_index("pz")
    greet_all(2, n)
    slot = 2 * (s // 2) + a
    parity = lax.rem(s, 2)
    remote = functools.partial(pltpu.make_async_remote_copy, device_id_type=MESH)
    halos = [
        remote(velocity, beside, halo_out.at[0], halo_in.at[0], device_id=(1 - a, s)),
        remote(velocity.at[:, lp - 1], near.at[0], halo_out.at[1], halo_in.at[1], device_id=(a, lax.rem(s + 1, n))),
        remote(velocity.at[:, 0], near.at[1], halo_out.at[2], halo_in.at[2], device_id=(a, lax.rem(s + n - 1, n))),
    ]
    for copy in halos:
        copy.start()

    def send(p):
        itself = (parity == a) & (p == s)
        copy = remote(back.at[p], home.at[slot], back_out.at[p], back_in.at[slot], device_id=(parity, p))
        return itself, copy, pltpu.make_async_copy(back.at[p], home.at[slot], back_in.at[slot])

    @pl.loop(0, n)
    def _(i):
        itself, copy, here = send(lax.rem(s + i, n))
        pl.when(itself)(here.start)
        pl.when(jnp.logical_not(itself))(copy.start)

    for copy in halos:
        copy.wait()
    lane = lax.broadcasted_iota(jnp.int32, (nz, nx), 1)
    has_below = (s > 0).astype(jnp.float32)
    has_above = (s < n - 1).astype(jnp.float32)

    def plane(y, ups, downs):
        dx, dy, dz = [], [], []
        for c in range(3):
            v, side = velocity[c, y], beside[c, y]
            ahead = jnp.where(lane == nx - 1, pltpu.roll(side, nx - 1, 1), pltpu.roll(v, nx - 1, 1))
            behind = jnp.where(lane == 0, pltpu.roll(side, 1, 1), pltpu.roll(v, 1, 1))
            dx.append(ahead - behind)
            dz.append(pltpu.roll(v, nz - 1, 0) - pltpu.roll(v, 1, 0))
            dy.append(ups[c] - downs[c])
        out[y] = tensor_norm(strain_of(dx, dy, dz))

    line = [near[0, c] * has_below for c in range(3)]
    plane(0, [velocity[c, 1] for c in range(3)], line)
    line = [near[1, c] * has_above for c in range(3)]
    plane(lp - 1, line, [velocity[c, lp - 2] for c in range(3)])

    @pl.loop(1, lp - 1)
    def _(y):
        plane(y, [velocity[c, y + 1] for c in range(3)], [velocity[c, y - 1] for c in range(3)])

    @pl.loop(0, n)
    def _(p):
        pltpu.make_async_copy(back.at[0], home.at[p], back_in.at[p]).wait()
        itself, copy, here = send(p)
        pl.when(jnp.logical_not(itself))(copy.wait_send)


def magnitude_kernel(centre, right, left, below, above, out):
    _, lp, nz, nx = centre.shape
    lane = lax.broadcasted_iota(jnp.int32, (nz, nx), 1)
    for y in range(lp):
        v = [centre[c, y] for c in range(3)]
        dx, dy, dz = [], [], []
        for c in range(3):
            ahead = jnp.where(lane == nx - 1, pltpu.roll(right[c, y], nx - 1, 1), pltpu.roll(v[c], nx - 1, 1))
            behind = jnp.where(lane == 0, pltpu.roll(left[c, y], 1, 1), pltpu.roll(v[c], 1, 1))
            dx.append(ahead - behind)
            dz.append(pltpu.roll(v[c], nz - 1, 0) - pltpu.roll(v[c], 1, 0))
            up = centre[c, y + 1] if y + 1 < lp else above[c, 0]
            down = centre[c, y - 1] if y else below[c, 0]
            dy.append(up - down)
        out[y] = tensor_norm(strain_of(dx, dy, dz))


def local(velocity, filter_inverse, filter_block, plane_bin):
    _, lp, nz, nx = velocity.shape
    n = lax.axis_size("pz")
    m = lax.axis_size("px")
    ny, zs = n * lp, nz // n
    win = zs + 4
    half = zs + 2
    shared = m == 2 and n % 2 == 0 and n > 2 and half == 2 * zs and 12 * half * (lp // 8) <= nx
    core = lax.axis_index("px")

    same = (filter_block[:, None] == filter_block[None, :]).astype(jnp.float32)
    masked = filter_inverse * same
    weights = masked / jnp.sum(masked, axis=1, keepdims=True)
    onehot = (plane_bin[:, None] == jnp.arange(nx, dtype=jnp.int32)[None, :]).astype(jnp.float32)

    if shared:
        turned = jnp.transpose(velocity, (2, 0, 1, 3)).reshape(nz, 3 * lp, nx)
        main = jnp.concatenate([turned[-2:], turned, turned[:2]], axis=0)
        edge = pl.pallas_call(
            functools.partial(edge_kernel, (half, lp, nx)),
            out_shape=jax.ShapeDtypeStruct((n // 2 + 1, 8, nx), jnp.float32),
        )(main)
        own, own_edge, other, other_edge = pl.pallas_call(
            functools.partial(outward_kernel, (n, half, lp)),
            out_shape=(
                jax.ShapeDtypeStruct((n, half, 3 * lp, nx), jnp.float32),
                jax.ShapeDtypeStruct((n, 8, nx), jnp.float32),
                jax.ShapeDtypeStruct((n, 2, 3 * lp, nx), jnp.float32),
                jax.ShapeDtypeStruct((n, 8, nx), jnp.float32),
            ),
            in_specs=[pl.BlockSpec(memory_space=pltpu.VMEM)] * 2,
            out_specs=(pl.BlockSpec(memory_space=pltpu.VMEM),) * 4,
            scratch_shapes=[pltpu.SemaphoreType.DMA((n,))] * 4 + [pltpu.SemaphoreType.DMA((2, n))] * 2,
            compiler_params=pltpu.CompilerParams(collective_id=0, has_side_effects=True),
        )(main, edge)
        fill, blocks = fill_from_halves, (core.astype(jnp.int32).reshape(1), own, own_edge, other, other_edge)
        specs = [pl.BlockSpec(memory_space=pltpu.SMEM)] + [pl.BlockSpec(memory_space=pltpu.VMEM)] * 4
    else:
        right = lax.ppermute(velocity, "px", [((i + 1) % m, i) for i in range(m)])
        left = right if m == 2 else lax.ppermute(velocity, "px", [(i, (i + 1) % m) for i in range(m)])
        below = lax.ppermute(velocity[:, -1:], "pz", [(i, i + 1) for i in range(n - 1)])
        above = lax.ppermute(velocity[:, :1], "pz", [(i + 1, i) for i in range(n - 1)])
        magnitude = pl.pallas_call(
            magnitude_kernel,
            out_shape=jax.ShapeDtypeStruct((lp, nz, nx), jnp.float32),
            cost_estimate=pl.CostEstimate(flops=60 * lp * nz * nx, bytes_accessed=40 * lp * nz * nx, transcendentals=0),
        )(velocity, right, left, below, above)
        turned = jnp.transpose(velocity, (0, 2, 1, 3))
        turned = jnp.concatenate([turned[:, -2:], turned, turned[:, :2]], axis=1)
        sent = jnp.stack([turned[:, t * zs : t * zs + win] for t in range(n)])
        own = lax.all_to_all(sent, "pz", split_axis=0, concat_axis=0, tiled=True)
        ahead = lax.ppermute(own, "px", [((i + 1) % m, i) for i in range(m)])
        behind = lax.ppermute(own, "px", [(i, (i + 1) % m) for i in range(m)])
        fill, blocks = fill_from_blocks, (own, ahead, behind)
        specs = [pl.BlockSpec(memory_space=pltpu.VMEM)] * 3

    rows = 6 * zs * lp
    back = pl.pallas_call(
        functools.partial(column_kernel, (n, win, lp, nx), fill, len(blocks)),
        out_shape=jax.ShapeDtypeStruct((n, rows + 8, nx), jnp.float32),
        in_specs=specs + [pl.BlockSpec(memory_space=pltpu.VMEM)] * 2,
        out_specs=pl.BlockSpec(memory_space=pltpu.VMEM),
        scratch_shapes=[
            pltpu.VMEM((3, win, ny + 16, 2 * nx), jnp.float32),
            pltpu.VMEM((21, ny, zs * nx), jnp.bfloat16),
            pltpu.VMEM((21, ny, zs * nx), jnp.bfloat16),
            pltpu.VMEM((21, ny, zs * nx), jnp.float32),
            pltpu.VMEM((ny, nx), jnp.float32),
            pltpu.VMEM((ny, nx), jnp.float32),
            pltpu.VMEM((ny, ny), jnp.bfloat16),
            pltpu.VMEM((ny, ny), jnp.bfloat16),
        ],
        compiler_params=pltpu.CompilerParams(vmem_limit_bytes=60 * 1024 * 1024),
    )(*blocks, weights, onehot)

    if shared:
        home, magnitude = pl.pallas_call(
            functools.partial(return_kernel, n),
            out_shape=(
                jax.ShapeDtypeStruct(back.shape, jnp.float32),
                jax.ShapeDtypeStruct((lp, nz, nx), jnp.float32),
            ),
            in_specs=[pl.BlockSpec(memory_space=pltpu.VMEM)] * 2,
            out_specs=(pl.BlockSpec(memory_space=pltpu.VMEM),) * 2,
            scratch_shapes=[
                pltpu.VMEM((3, lp, nz, nx), jnp.float32),
                pltpu.VMEM((2, 3, nz, nx), jnp.float32),
                pltpu.SemaphoreType.DMA((n,)),
                pltpu.SemaphoreType.DMA((n,)),
                pltpu.SemaphoreType.DMA((3,)),
                pltpu.SemaphoreType.DMA((3,)),
            ],
            compiler_params=pltpu.CompilerParams(collective_id=1, has_side_effects=True),
        )(back, velocity)
        totals = jnp.sum(home[:, rows:], axis=0)
        totals = totals + lax.ppermute(totals, "px", [(0, 1), (1, 0)])
    else:
        home = lax.all_to_all(back, "pz", split_axis=0, concat_axis=0, tiled=True)
        totals = lax.psum(jnp.sum(home[:, rows:], axis=0), "px")
    stress = home[:, :rows].reshape(n, 6, zs, lp, nx)
    leonard = jnp.transpose(stress, (1, 3, 0, 2, 4)).reshape(6, lp, nz, nx)
    numer, denom = totals[0, :NBIN], totals[4, :NBIN]
    cells = nx * m * nz
    per_bin = numer / jnp.maximum(denom, jnp.float32(cells))
    coefficient = jnp.dot(onehot[:, :NBIN], per_bin, precision=lax.Precision.HIGHEST)
    local_coef = lax.dynamic_slice_in_dim(coefficient, lax.axis_index("pz") * lp, lp, 0)
    viscosity = local_coef[:, None, None] * magnitude
    return (leonard, viscosity, coefficient)


def solution(mesh):
    return jax.shard_map(
        local,
        mesh=mesh,
        in_specs=(P(None, "pz", None, "px"), P(), P(), P()),
        out_specs=(P(None, "pz", None, "px"), P("pz", None, "px"), P()),
        check_vma=False,
    )
```
